32 devices in a mesh: dp: 8 (over z, y), tensor: 4 (over x, core).
Axes of the slice: x: 2, y: 2, z: 4, core: 2. Of those that a mesh axis runs over, the one named last changes fastest.
Arguments:
- tokens: bfloat16 [16384, 4096], P('dp', 'tensor'), may hold values from -6 to 6
- cotangent: bfloat16 [16384, 1536], P('dp', 'tensor'), may hold values from -0.059814453 to 0.059814453
- seg_start: int32 [8, 2], P('dp'), may hold values from 0 to 1024, as said below
- seg_length: int32 [8, 2], P('dp'), may hold values from 0 to 1024, as said below
Outputs:
- weight_grad: float32 [4096, 2, 1536], P('dp', None, 'tensor')
The draws below stay inside these ranges and needn't reach their ends.
Inputs may be any that keep to these rules, and one draw needn't show every extreme that they name: Within each index of dp the 2 segments lie in expert order, packed from row 0 without gaps: seg_start is the running sum of seg_length before each expert. `seg_length`: each length is at most 1024; in every draw some expert on some index of dp has exactly 1024 rows. Rows after the last segment belong to no expert.
All inputs are finite; a program needn't handle non-finite values.
Results may differ from the reference program's by a relative error of at most 0.0003.
Values may be sent and summed in bfloat16 or wider, within the bound.
A program may use at most 128 MiB of HBM per device.

```python
import jax
import jax.numpy as jnp
from jax import lax

D = 4096
FF = 1536
E_W = 2
CAP = 1024
TOKENS = 16384
N_DP = 8


def segment_bounds(key):
    keys = jax.random.split(jax.random.fold_in(key, 7), 4)
    load = jax.random.randint(keys[0], (N_DP, 1), 1, 5)
    lower = load * CAP // 8
    upper = load * CAP // 4 + 1
    draws = jax.random.randint(keys[1], (N_DP, E_W), 0, 1 << 30)
    length = lower + draws % (upper - lower)
    busy_device = jax.random.randint(keys[2], (), 0, N_DP)
    busy_expert = jax.random.randint(keys[3], (), 0, E_W)
    hit = (jnp.arange(N_DP)[:, None] == busy_device) & (jnp.arange(E_W)[None, :] == busy_expert)
    length = jnp.where(hit, CAP, length)
    start = jnp.cumsum(length, axis=1) - length
    return (start.astype(jnp.int32), length.astype(jnp.int32))


def draw_seg_start(key, part):
    return segment_bounds(key)[0]


def draw_seg_length(key, part):
    return segment_bounds(key)[1]


def with_spikes(values, rng, source, target, shards_of, factor):
    owner, partner = [(jnp.arange(values.shape[axis_at]) // (values.shape[axis_at] // shards_of)).reshape([-1 if axis == axis_at else 1 for axis in range(values.ndim)]) for axis_at in (source, target)]
    chosen = jax.random.permutation(rng, shards_of)[partner]
    strong = (owner == chosen) | (owner == (partner + shards_of // 2) % shards_of)
    return jnp.where(strong, factor * values, values)


def level_of(own_key, extent, shards, low, high):
    factor_of = 1.0
    for position, parts in shards:
        steps = jax.random.uniform(jax.random.fold_in(jax.random.fold_in(own_key, 6), position), (parts,), jnp.float32, low / len(shards), high / len(shards))
        factor_of = factor_of * jnp.repeat(jnp.exp(steps), extent[position] // parts).reshape((-1,) + (1,) * (len(extent) - 1 - position))
    return factor_of


def noise(key, extent, scale, bound, cuts=(), kind=jnp.bfloat16):
    values = jax.random.normal(key, extent, jnp.float32) * scale
    if len(cuts) > 0:
        values = level_of(key, extent, cuts, -0.22, 0.18) * values
    return jnp.clip(values, min=-bound, max=bound).astype(kind)


def bell_draw_with(stream_key, shape, width, bound, cuts, heavy, kind=jnp.bfloat16):
    drawn = width * jax.random.normal(stream_key, shape, jnp.float32)
    if cuts:
        drawn = drawn * level_of(stream_key, shape, cuts, -0.22, 0.18)
    return jnp.clip(with_spikes(drawn, jax.random.fold_in(stream_key, 3), *heavy), -bound, bound).astype(kind)


def setup_inputs(seed: int = 0) -> dict:
    splits = jax.random.split(jax.random.key(seed), 5)
    tokens = bell_draw_with(splits[0], (TOKENS, D), 1.0, 6.0, ((0, 8), (1, 4)), (0, 1, 8, 2.0))
    cotangent = noise(splits[1], (TOKENS, FF), 0.01, 0.059814453, ((0, 8), (1, 4)))
    seg_start = draw_seg_start(jax.random.fold_in(splits[4], 71), 0)
    seg_length = draw_seg_length(jax.random.fold_in(splits[4], 71), 0)
    return dict(tokens=tokens, cotangent=cotangent, seg_start=seg_start, seg_length=seg_length)


def reference(tokens, cotangent, seg_start, seg_length):
    tok = E_W * CAP

    def peer(total, index):
        rows_x = lax.dynamic_slice_in_dim(tokens, index * tok, tok, 0)
        rows_g = lax.dynamic_slice_in_dim(cotangent, index * tok, tok, 0)
        terms = []
        for expert in range(E_W):
            start = seg_start[index, expert].astype(jnp.int32)
            length = seg_length[index, expert].astype(jnp.int32)
            first = jnp.minimum(start, tok - CAP).astype(jnp.int32)
            rows = first + jnp.arange(CAP, dtype=jnp.int32)
            keep = (rows >= start) & (rows < start + length)
            block_x = lax.dynamic_slice_in_dim(rows_x, first, CAP, 0)
            block_g = lax.dynamic_slice_in_dim(rows_g, first, CAP, 0)
            block_g = jnp.where(keep[:, None], block_g, jnp.zeros_like(block_g))
            terms.append(jnp.dot(block_x.T, block_g, preferred_element_type=jnp.float32))
        return total + jnp.stack(terms, 1), None

    start_total = jnp.zeros((D, E_W, FF), jnp.float32)
    total, unused = lax.scan(peer, start_total, jnp.arange(N_DP, dtype=jnp.int32))
    return total
```

```python
import functools

import jax
import jax.numpy as jnp
from jax import lax
from jax.experimental import pallas as pl
from jax.experimental.pallas import tpu as pltpu
from jax.sharding import PartitionSpec as P

CAP = 1024
SUB = 128
MESH = pl.DeviceIdType.MESH


def block_term(columns, grads, lower, upper, size):
    total_rows = columns.shape[0]
    first = jnp.minimum(lower, total_rows - size)
    rows = first + jnp.arange(size, dtype=jnp.int32)
    keep = (rows >= lower) & (rows < upper)
    block_x = lax.dynamic_slice_in_dim(columns, first, size, 0)
    block_g = lax.dynamic_slice_in_dim(grads, first, size, 0)
    block_g = jnp.where(keep[:, None], block_g, jnp.zeros_like(block_g))
    return lax.dot_general(
        block_x, block_g, (((0,), (0,)), ((), ())), preferred_element_type=jnp.float32
    )


def plain_device(tokens, cotangent, seg_start, seg_length):
    whole = lax.all_gather(tokens, "tensor", axis=1, tiled=True)
    terms = []
    for expert in range(seg_start.shape[1]):
        start = seg_start[0, expert]
        upper = start + seg_length[0, expert]
        terms.append(block_term(whole, cotangent, start, upper, CAP))
    return lax.psum_scatter(jnp.stack(terms, 1), "dp", scatter_dimension=0, tiled=True)


def grad_kernel(
    n_dp, n_t, experts, tok_ref, cot_ref, info_ref, out_ref,
    cot_in, info_in, gt, tok, part, recv_r, recv_l,
    tok_send, tok_recv, small_send, small_recv, r_send, r_recv, l_send, l_recv,
):
    d = lax.axis_index("dp")
    t = lax.axis_index("tensor")
    line = n_dp // 2
    z, y = d // 2, d % 2
    rows, width = tok_ref.shape
    ff = cot_ref.shape[1]
    half = width // 2
    n_sub = half // SUB
    others = n_t // 2 - 1
    partner = (d, t + 1 - 2 * (t % 2))
    pair = (d + 1 - 2 * y, t)
    across = [(d, (t + 2 * k) % n_t) for k in range(1, others + 1)]

    barrier = pltpu.get_barrier_semaphore()
    for device in [partner, pair] + across:
        pl.semaphore_signal(barrier, inc=1, device_id=device, device_id_type=MESH)

    @pl.when(z > 0)
    def _():
        pl.semaphore_signal(barrier, inc=1, device_id=(d - 2, t), device_id_type=MESH)

    @pl.when(z < line - 1)
    def _():
        pl.semaphore_signal(barrier, inc=1, device_id=(d + 2, t), device_id_type=MESH)

    ends = jnp.where(z > 0, 1, 0) + jnp.where(z < line - 1, 1, 0)
    pl.semaphore_wait(barrier, 2 + others + ends)

    def slot(r, j, q):
        return tok.at[r, j, :, pl.ds(pl.multiple_of(q * SUB, SUB), SUB)]

    def own(parity, j):
        return tok_ref.at[:, pl.ds(pl.multiple_of(parity * half + j * SUB, SUB), SUB)]

    def send(src, r, q, j, kind, device):
        return pltpu.make_async_remote_copy(
            src_ref=src, dst_ref=slot(r, j, q), send_sem=tok_send.at[kind, j],
            recv_sem=tok_recv.at[r, q, j], device_id=device, device_id_type=MESH,
        )

    def arrived(r, q, j):
        send(slot(r, j, q), r, q, j, 0, partner).wait_recv()

    info_copy = pltpu.make_async_remote_copy(
        src_ref=info_ref, dst_ref=info_in, send_sem=small_send.at[0],
        recv_sem=small_recv.at[0], device_id=pair, device_id_type=MESH,
    )
    cot_copy = pltpu.make_async_remote_copy(
        src_ref=cot_ref, dst_ref=cot_in, send_sem=small_send.at[1],
        recv_sem=small_recv.at[1], device_id=pair, device_id_type=MESH,
    )
    info_copy.start()
    cot_copy.start()
    for j in range(n_sub):
        send(own(1 - y, j), 1, t, j, 1, pair).start()
        for k, device in enumerate(across):
            send(own(y, j), 0, t, j, 3 + 4 * k, device).start()
        send(own(y, j), 0, t, j, 0, partner).start()
    for j in range(n_sub):
        tok[0, j, :, pl.ds(pl.multiple_of(t * SUB, SUB), SUB)] = tok_ref[
            :, pl.ds(pl.multiple_of(y * half + j * SUB, SUB), SUB)
        ]

    chunk = 256

    def masked(r, grads, info):
        @pl.loop(0, rows // chunk)
        def _(i):
            at = pl.ds(pl.multiple_of(i * chunk, chunk), chunk)
            block = grads[at, :].astype(jnp.float32).T
            col = i * chunk + lax.broadcasted_iota(jnp.int32, (ff, chunk), 1)
            for e in range(experts):
                keep = (col >= info[2 * e : 2 * e + 1, :]) & (col < info[2 * e + 1 : 2 * e + 2, :])
                gt[r, e * ff : (e + 1) * ff, at] = jnp.where(keep, block, 0.0).astype(gt.dtype)

    masked(0, cot_ref, info_ref)
    info_copy.wait_recv()
    cot_copy.wait_recv()
    masked(1, cot_in, info_in)

    def from_pair(j):
        arrived(1, t, j)
        for k, device in enumerate(across):
            send(slot(1, j, t), 1, t, j, 4 + 4 * k, device).start()
        send(slot(1, j, t), 1, t, j, 2, partner).start()

    def right(j, q):
        return pltpu.make_async_remote_copy(
            src_ref=part.at[j, q], dst_ref=recv_r.at[j, q], send_sem=r_send.at[j, q],
            recv_sem=r_recv.at[j, q], device_id=(d + 2, t), device_id_type=MESH,
        )

    def left(j, q):
        return pltpu.make_async_remote_copy(
            src_ref=part.at[j, q], dst_ref=recv_l.at[j, q], send_sem=l_send.at[j, q],
            recv_sem=l_recv.at[j, q], device_id=(d - 2, t), device_id_type=MESH,
        )

    tile = 256
    from_pair(0)

    @pl.loop(0, n_sub)
    def _(j):
        @pl.when(j + 1 < n_sub)
        def _():
            from_pair(j + 1)

        for r in range(2):
            for k in range(others):
                q = (t + 2 * (k + 1)) % n_t
                arrived(r, q, j)
                send(slot(r, j, q), r, q, j, 5 + 4 * k + r, partner).start()
        for r in range(2):
            for k in range(others + 1):
                arrived(r, (partner[1] + 2 * k) % n_t, j)

        @pl.loop(0, experts * ff // tile)
        def _(m):
            at = pl.ds(pl.multiple_of(m * tile, tile), tile)
            total = jnp.dot(gt[0, at, :], tok[0, j], preferred_element_type=jnp.float32)
            total += jnp.dot(gt[1, at, :], tok[1, j], preferred_element_type=jnp.float32)
            for q in range(n_t):
                part[j, q, at, :] = total[:, q * SUB : (q + 1) * SUB]

        for q in range(n_t):
            @pl.when((z == line - 1) & (q < z))
            def _():
                left(j, q).start()
        for q in reversed(range(n_t)):
            @pl.when((z == 0) & (q > z))
            def _():
                right(j, q).start()

    @pl.loop(0, n_sub)
    def _(j):
        order = []
        for q in range(n_t):
            for o in (n_t - 1 - q, q):
                if o not in order:
                    order.append(o)
        for q in order:
            @pl.when((q > z) & (z > 0))
            def _():
                right(j, q).wait_recv()
                part[j, q] = part[j, q] + recv_r[j, q]
                right(j, q).start()

            @pl.when((q < z) & (z < line - 1))
            def _():
                left(j, q).wait_recv()
                part[j, q] = part[j, q] + recv_l[j, q]
                left(j, q).start()

    @pl.loop(0, n_sub)
    def _(j):
        out_ref[j] = part[j, z]

        @pl.when(z > 0)
        def _():
            right(j, z).wait_recv()
            out_ref[j] += recv_r[j, z]

        @pl.when(z < line - 1)
        def _():
            left(j, z).wait_recv()
            out_ref[j] += recv_l[j, z]

    @pl.loop(0, n_sub)
    def _(j):
        for q in range(n_t):
            @pl.when(q > z)
            def _():
                right(j, q).wait_send()

            @pl.when(q < z)
            def _():
                left(j, q).wait_send()
        for kind in range(3 + 4 * others):
            send(slot(0, j, t), 0, t, j, kind, partner).wait_send()
    info_copy.wait_send()
    cot_copy.wait_send()


def kernel_device(n_dp, n_t, tokens, cotangent, seg_start, seg_length):
    rows, width = tokens.shape
    ff = cotangent.shape[1]
    experts = seg_start.shape[1]
    half = width // 2
    n_sub = half // SUB
    others = n_t // 2 - 1
    bounds = jnp.stack([seg_start[0], seg_start[0] + seg_length[0]], 1).reshape(-1)
    pad = -(2 * experts) % 8
    info = jnp.broadcast_to(jnp.pad(bounds, (0, pad))[:, None], (2 * experts + pad, 256))
    dma = pltpu.SemaphoreType.DMA
    blocks = (n_sub, n_t, experts * ff, SUB)
    vmem = pl.BlockSpec(memory_space=pltpu.VMEM)
    out = pl.pallas_call(
        functools.partial(grad_kernel, n_dp, n_t, experts),
        out_shape=jax.ShapeDtypeStruct((n_sub, experts * ff, SUB), jnp.float32),
        in_specs=[vmem] * 3,
        out_specs=vmem,
        scratch_shapes=[
            pltpu.VMEM((rows, ff), cotangent.dtype),
            pltpu.VMEM(info.shape, jnp.int32),
            pltpu.VMEM((2, experts * ff, rows), cotangent.dtype),
            pltpu.VMEM((2, n_sub, rows, n_t * SUB), tokens.dtype),
            pltpu.VMEM(blocks, jnp.float32),
            pltpu.VMEM(blocks, jnp.float32),
            pltpu.VMEM(blocks, jnp.float32),
            dma((3 + 4 * others, n_sub)),
            dma((2, n_t, n_sub)),
            dma((2,)),
            dma((2,)),
            dma((n_sub, n_t)),
            dma((n_sub, n_t)),
            dma((n_sub, n_t)),
            dma((n_sub, n_t)),
        ],
        compiler_params=pltpu.CompilerParams(
            collective_id=0, has_side_effects=True, vmem_limit_bytes=67043328
        ),
    )(tokens, cotangent, info)
    out = out.reshape(n_sub, experts, ff, SUB)
    return out.transpose(0, 3, 1, 2).reshape(half, experts, ff)


def solution(mesh):
    n_dp, n_t = mesh.shape["dp"], mesh.shape["tensor"]
    body = plain_device
    if n_dp == 2 * n_t:
        body = functools.partial(kernel_device, n_dp, n_t)
    in_specs = (P("dp", "tensor"), P("dp", "tensor"), P("dp", None), P("dp", None))
    out_specs = P("dp", None, "tensor")
    return jax.shard_map(
        body, mesh=mesh, in_specs=in_specs, out_specs=out_specs, check_vma=False
    )
```

```python
import functools

import jax
import jax.numpy as jnp
from jax import lax
from jax.experimental import pallas as pl
from jax.experimental.pallas import tpu as pltpu
from jax.sharding import PartitionSpec as P

CAP = 1024
SUB = 128
MESH = pl.DeviceIdType.MESH


def block_term(columns, grads, lower, upper, size):
    total_rows = columns.shape[0]
    first = jnp.minimum(lower, total_rows - size)
    rows = first + jnp.arange(size, dtype=jnp.int32)
    keep = (rows >= lower) & (rows < upper)
    block_x = lax.dynamic_slice_in_dim(columns, first, size, 0)
    block_g = lax.dynamic_slice_in_dim(grads, first, size, 0)
    block_g = jnp.where(keep[:, None], block_g, jnp.zeros_like(block_g))
    return lax.dot_general(
        block_x, block_g, (((0,), (0,)), ((), ())), preferred_element_type=jnp.float32
    )


def plain_device(tokens, cotangent, seg_start, seg_length):
    whole = lax.all_gather(tokens, "tensor", axis=1, tiled=True)
    terms = []
    for expert in range(seg_start.shape[1]):
        start = seg_start[0, expert]
        upper = start + seg_length[0, expert]
        terms.append(block_term(whole, cotangent, start, upper, CAP))
    return lax.psum_scatter(jnp.stack(terms, 1), "dp", scatter_dimension=0, tiled=True)


def plan(n_sub, n_ff):
    events = []
    for i in range(max(n_sub, n_ff)):
        events += [("cot", i)] * (i < n_ff) + [("tok", i)] * (i < n_sub)
    groups = []
    for kind, i in events:
        if kind == "tok":
            groups.append((i, []))
    have = {i: max(0, min(n_ff, i + 2)) for i in range(n_sub)}
    seen = set()
    for i, added in groups:
        for j in range(i + 1):
            for f in range(have[i]):
                if (j, f) not in seen:
                    seen.add((j, f))
                    added.append((j, f))
    for j in range(n_sub):
        for f in range(n_ff):
            if (j, f) not in seen:
                groups[-1][1].append((j, f))
    return events, groups, have


def grad_kernel(
    n_dp, n_t, experts, tok_ref, cot_ref, info_ref, out_ref,
    cot_in, info_in, gt, tok, part, recv_r, recv_l,
    tok_send, tok_recv, small_send, small_recv, r_send, r_recv, l_send, l_recv,
):
    d = lax.axis_index("dp")
    t = lax.axis_index("tensor")
    line = n_dp // 2
    z, y = d // 2, d % 2
    rows, width = tok_ref.shape
    ff = cot_ref.shape[1]
    half = width // 2
    n_sub, n_ff = half // SUB, ff // SUB
    n_steps = n_sub * n_ff
    others = n_t // 2 - 1
    partner = (d, t + 1 - 2 * (t % 2))
    pair = (d + 1 - 2 * y, t)
    across = [(d, (t + 2 * k) % n_t) for k in range(1, others + 1)]

    barrier = pltpu.get_barrier_semaphore()
    for device in [partner, pair] + across:
        pl.semaphore_signal(barrier, inc=1, device_id=device, device_id_type=MESH)

    @pl.when(z > 0)
    def _():
        pl.semaphore_signal(barrier, inc=1, device_id=(d - 2, t), device_id_type=MESH)

    @pl.when(z < line - 1)
    def _():
        pl.semaphore_signal(barrier, inc=1, device_id=(d + 2, t), device_id_type=MESH)

    ends = jnp.where(z > 0, 1, 0) + jnp.where(z < line - 1, 1, 0)
    pl.semaphore_wait(barrier, 2 + others + ends)

    def slot(r, j, q):
        return tok.at[r, j, :, pl.ds(pl.multiple_of(q * SUB, SUB), SUB)]

    def own(parity, j):
        return tok_ref.at[:, pl.ds(pl.multiple_of(parity * half + j * SUB, SUB), SUB)]

    def send(src, r, q, j, kind, device):
        return pltpu.make_async_remote_copy(
            src_ref=src, dst_ref=slot(r, j, q), send_sem=tok_send.at[kind, j],
            recv_sem=tok_recv.at[r, q, j], device_id=device, device_id_type=MESH,
        )

    def arrived(r, q, j):
        send(slot(r, j, q), r, q, j, 0, partner).wait_recv()

    info_copy = pltpu.make_async_remote_copy(
        src_ref=info_ref, dst_ref=info_in, send_sem=small_send.at[n_ff],
        recv_sem=small_recv.at[n_ff], device_id=pair, device_id_type=MESH,
    )

    def cot_copy(f):
        at = pl.ds(f * SUB, SUB)
        return pltpu.make_async_remote_copy(
            src_ref=cot_ref.at[:, at], dst_ref=cot_in.at[:, at], send_sem=small_send.at[f],
            recv_sem=small_recv.at[f], device_id=pair, device_id_type=MESH,
        )

    def own_across(j):
        for k, device in enumerate(across):
            send(own(y, j), 0, t, j, 3 + 4 * k, device).start()

    events, groups, have = plan(n_sub, n_ff)
    info_copy.start()
    for kind, i in events:
        if kind == "cot":
            cot_copy(i).start()
        else:
            send(own(1 - y, i), 1, t, i, 1, pair).start()
    for j in range(min(2, n_sub)):
        own_across(j)
    for j in range(n_sub):
        send(own(y, j), 0, t, j, 0, partner).start()
    for j in range(n_sub):
        tok[0, j, :, pl.ds(pl.multiple_of(t * SUB, SUB), SUB)] = tok_ref[
            :, pl.ds(pl.multiple_of(y * half + j * SUB, SUB), SUB)
        ]

    chunk = 256
    deep = experts * SUB

    def masked(r, grads, info, f):
        @pl.loop(0, rows // chunk)
        def _(i):
            at = pl.ds(pl.multiple_of(i * chunk, chunk), chunk)
            block = grads[at, f * SUB : (f + 1) * SUB].astype(jnp.float32).T
            col = i * chunk + lax.broadcasted_iota(jnp.int32, (SUB, chunk), 1)
            for e in range(experts):
                keep = (col >= info[2 * e : 2 * e + 1, :]) & (col < info[2 * e + 1 : 2 * e + 2, :])
                gt[r, f * deep + e * SUB : f * deep + (e + 1) * SUB, at] = jnp.where(
                    keep, block, 0.0
                ).astype(gt.dtype)

    for f in range(n_ff):
        masked(0, cot_ref, info_ref, f)
    info_copy.wait_recv()

    def right(s, q):
        return pltpu.make_async_remote_copy(
            src_ref=part.at[s, q], dst_ref=recv_r.at[s, q], send_sem=r_send.at[s, q],
            recv_sem=r_recv.at[s, q], device_id=(d + 2, t), device_id_type=MESH,
        )

    def left(s, q):
        return pltpu.make_async_remote_copy(
            src_ref=part.at[s, q], dst_ref=recv_l.at[s, q], send_sem=l_send.at[s, q],
            recv_sem=l_recv.at[s, q], device_id=(d - 2, t), device_id_type=MESH,
        )

    def middle(s):
        u, v = s - (z - 1), s - (line - 2 - z)
        for q in reversed(range(n_t)):
            @pl.when((q > z) & (z > 0) & (u >= 0) & (u < n_steps))
            def _():
                right(u, q).wait_recv()
                part[u, q] = part[u, q] + recv_r[u, q]
                right(u, q).start()
        for q in range(n_t):
            @pl.when((q < z) & (z < line - 1) & (v >= 0) & (v < n_steps))
            def _():
                left(v, q).wait_recv()
                part[v, q] = part[v, q] + recv_l[v, q]
                left(v, q).start()

    def from_pair(j):
        arrived(1, t, j)
        for k, device in enumerate(across):
            send(slot(1, j, t), 1, t, j, 4 + 4 * k, device).start()
        send(slot(1, j, t), 1, t, j, 2, partner).start()
        if j + 2 < n_sub:
            own_across(j + 2)

    def from_across(r, j):
        for k in range(others):
            q = (t + 2 * (k + 1)) % n_t
            arrived(r, q, j)
            send(slot(r, j, q), r, q, j, 5 + 4 * k + r, partner).start()

    blocks_in, subs_in, s, hops = 0, 0, 0, 0
    places = []
    last = []
    for i, steps in groups:
        for j in range(subs_in, min(n_sub, i + 1 + (blocks_in == n_ff))):
            while blocks_in < min(n_ff, j + 1):
                cot_copy(blocks_in).wait_recv()
                masked(1, cot_in, info_in, blocks_in)
                blocks_in += 1
            from_pair(j)
            from_across(0, j)
            subs_in = j + 1
        while blocks_in < have[i]:
            cot_copy(blocks_in).wait_recv()
            masked(1, cot_in, info_in, blocks_in)
            blocks_in += 1
        from_across(1, i)
        for r in range(2):
            for k in range(others + 1):
                arrived(r, (partner[1] + 2 * k) % n_t, i)
        for j, f in steps:
            at = pl.ds(f * deep, deep)
            total = jnp.dot(gt[0, at, :], tok[0, j], preferred_element_type=jnp.float32)
            total += jnp.dot(gt[1, at, :], tok[1, j], preferred_element_type=jnp.float32)
            for q in range(n_t):
                part[s, q] = total[:, q * SUB : (q + 1) * SUB]
            for q in range(n_t):
                @pl.when((z == line - 1) & (q < z))
                def _():
                    left(s, q).start()
            for q in reversed(range(n_t)):
                @pl.when((z == 0) & (q > z))
                def _():
                    right(s, q).start()
            places.append((j, f))
            s += 1
        last.append(s)
        if len(last) > 1:
            pl.loop(hops, last[-2])(middle)
            hops = last[-2]
    pl.loop(hops, n_steps + line - 2)(middle)

    for s, (j, f) in enumerate(places):
        here = j * n_ff + f
        out_ref[here] = part[s, z]

        @pl.when(z > 0)
        def _():
            right(s, z).wait_recv()
            out_ref[here] += recv_r[s, z]

        @pl.when(z < line - 1)
        def _():
            left(s, z).wait_recv()
            out_ref[here] += recv_l[s, z]

    @pl.loop(0, n_steps)
    def _(s):
        for q in range(n_t):
            @pl.when(q > z)
            def _():
                right(s, q).wait_send()

            @pl.when(q < z)
            def _():
                left(s, q).wait_send()

    @pl.loop(0, n_sub)
    def _(j):
        for kind in range(3 + 4 * others):
            send(slot(0, j, t), 0, t, j, kind, partner).wait_send()
    for f in range(n_ff):
        cot_copy(f).wait_send()
    info_copy.wait_send()


def kernel_device(n_dp, n_t, tokens, cotangent, seg_start, seg_length):
    rows, width = tokens.shape
    ff = cotangent.shape[1]
    experts = seg_start.shape[1]
    half = width // 2
    n_sub = half // SUB
    others = n_t // 2 - 1
    bounds = jnp.stack([seg_start[0], seg_start[0] + seg_length[0]], 1).reshape(-1)
    pad = -(2 * experts) % 8
    info = jnp.broadcast_to(jnp.pad(bounds, (0, pad))[:, None], (2 * experts + pad, 256))
    dma = pltpu.SemaphoreType.DMA
    n_ff = ff // SUB
    blocks = (n_sub * n_ff, n_t, experts * SUB, SUB)
    vmem = pl.BlockSpec(memory_space=pltpu.VMEM)
    out = pl.pallas_call(
        functools.partial(grad_kernel, n_dp, n_t, experts),
        out_shape=jax.ShapeDtypeStruct((n_sub * n_ff, experts * SUB, SUB), jnp.float32),
        in_specs=[vmem] * 3,
        out_specs=vmem,
        scratch_shapes=[
            pltpu.VMEM((rows, ff), cotangent.dtype),
            pltpu.VMEM(info.shape, jnp.int32),
            pltpu.VMEM((2, experts * ff, rows), cotangent.dtype),
            pltpu.VMEM((2, n_sub, rows, n_t * SUB), tokens.dtype),
            pltpu.VMEM(blocks, jnp.float32),
            pltpu.VMEM(blocks, jnp.float32),
            pltpu.VMEM(blocks, jnp.float32),
            dma((3 + 4 * others, n_sub)),
            dma((2, n_t, n_sub)),
            dma((n_ff + 1,)),
            dma((n_ff + 1,)),
            dma((n_sub * n_ff, n_t)),
            dma((n_sub * n_ff, n_t)),
            dma((n_sub * n_ff, n_t)),
            dma((n_sub * n_ff, n_t)),
        ],
        compiler_params=pltpu.CompilerParams(
            collective_id=0, has_side_effects=True, vmem_limit_bytes=67043328
        ),
    )(tokens, cotangent, info)
    out = out.reshape(n_sub, n_ff, experts, SUB, SUB)
    return out.transpose(0, 4, 2, 1, 3).reshape(half, experts, ff)


def solution(mesh):
    n_dp, n_t = mesh.shape["dp"], mesh.shape["tensor"]
    body = plain_device
    if n_dp == 2 * n_t:
        body = functools.partial(kernel_device, n_dp, n_t)
    in_specs = (P("dp", "tensor"), P("dp", "tensor"), P("dp", None), P("dp", None))
    out_specs = P("dp", None, "tensor")
    return jax.shard_map(
        body, mesh=mesh, in_specs=in_specs, out_specs=out_specs, check_vma=False
    )
```
